32 devices in a mesh: grp: 8 (over y, x, core), sp: 4 (over z).
Axes of the slice: x: 2, y: 2, z: 4, core: 2. Of those that a mesh axis runs over, the one named last changes fastest.
Arguments:
- latents: bfloat16 [8, 512, 3072], P('grp', 'sp'), may hold values from -6 to 6
- timestep: int32 [8], P('grp'), may hold values from 0 to 999
- w_mod: bfloat16 [256, 9216], replicated, may hold values from -0.375 to 0.375
- w_qkv: bfloat16 [4, 3072, 384], P('sp', 'grp'), may hold values from -2 to 2
- w_out: bfloat16 [4, 128, 3072], P('sp', 'grp'), may hold values from -0.5 to 0.5
Outputs:
- update: bfloat16 [8, 512, 3072], P('grp', 'sp')
The draws below stay inside these ranges and needn't reach their ends.
All inputs are finite; a program needn't handle non-finite values.
Results may differ from the reference program's by a relative error of at most 0.012.
Values may be sent and summed in bfloat16 or wider, within the bound.
No kernel may reach another device: no remote copies, remote signals or barrier semaphores. Data moves between devices by JAX's collectives and lax.ppermute only.
A program may use at most 128 MiB of HBM per device.

```python
import math
import jax
import jax.numpy as jnp
from jax import lax

D = 3072
HS = 128
FREQ = 256
H = 4
LEN = 512
IMAGES = 8


def draw_w_qkv(key, part):
    first, second, third = jax.random.split(jax.random.fold_in(key, 17), 3)
    base = 1.0 / math.sqrt(D)
    query_part = jax.random.normal(first, (H, D, HS), jnp.float32) * (1.5 * base)
    value_part = jax.random.normal(third, (H, D, HS), jnp.float32) * base
    key_part = jax.random.normal(second, (H, D, HS), jnp.float32) * base
    whole = jnp.concatenate([query_part, key_part, value_part], axis=2)
    return jnp.clip(whole, -2.0, 2.0).astype(jnp.bfloat16)


def plant(array, stream_key, smallest, top_value):
    spot = [jax.random.randint(jax.random.fold_in(stream_key, axis), (), 0, length) for axis, length in enumerate(array.shape)]
    main_axis = array.shape.index(max(array.shape))
    next_to = spot[:main_axis] + [(spot[main_axis] + 1) % array.shape[main_axis]] + spot[main_axis + 1:]
    return array.at[tuple(spot)].set(smallest).at[tuple(next_to)].set(top_value)


def shard_levels(rng, shape, cuts, low, high):
    level, own = 1.0, jax.random.fold_in(rng, 6)
    for dim, shards_of in cuts:
        steps = jnp.exp(jax.random.uniform(jax.random.fold_in(own, dim), (shards_of,), jnp.float32, low / len(cuts), high / len(cuts)))
        level = level * jnp.repeat(steps, shape[dim] // shards_of).reshape([-1 if axis == dim else 1 for axis in range(len(shape))])
    return level


def centred(stream_key, shape, scale, limit, cuts=(), held_as=jnp.bfloat16):
    array = jax.random.normal(stream_key, shape, jnp.float32) * scale
    if len(cuts) > 0:
        array = shard_levels(stream_key, shape, cuts, -0.22, 0.18) * array
    return jnp.clip(array, min=-limit, max=limit).astype(held_as)


def setup_inputs(seed: int = 0) -> dict:
    arg_keys = jax.random.split(jax.random.key(seed), 6)
    latents = centred(arg_keys[0], (IMAGES, LEN, D), 1.0, 6.0, ((0, 8), (1, 4)))
    timestep = plant(jax.random.randint(arg_keys[1], (IMAGES,), 0, 1000), jax.random.fold_in(arg_keys[1], 1), 0, 999).astype(jnp.int32)
    w_mod = centred(arg_keys[2], (FREQ, 3 * D), FREQ ** -0.5, 0.375)
    w_qkv = draw_w_qkv(jax.random.fold_in(arg_keys[5], 71), 0)
    w_out = centred(arg_keys[4], (H, HS, D), HS ** -0.5, 0.5, ((0, 4), (1, 8)))
    return {"latents": latents, "timestep": timestep, "w_mod": w_mod, "w_qkv": w_qkv, "w_out": w_out}


def modulation(timestep, w_mod):
    half_freq = w_mod.shape[0] // 2
    freqs = jnp.exp(-math.log(10000.0) * jnp.arange(half_freq, dtype=jnp.float32) / half_freq)
    angles = timestep.astype(jnp.float32)[:, None] * freqs[None, :]
    embed = jnp.concatenate([jnp.cos(angles), jnp.sin(angles)], axis=1).astype(jnp.bfloat16)
    return jnp.dot(embed, w_mod, preferred_element_type=jnp.float32)

def normalize(latents, shift, scale):
    values = latents.astype(jnp.float32)
    center = lax.optimization_barrier(jnp.mean(values, axis=-1, keepdims=True))
    spread = lax.optimization_barrier(jnp.mean((values - center) ** 2, axis=-1, keepdims=True))
    normed = (values - center) * lax.rsqrt(spread + 1e-06)
    return (normed * (1.0 + scale[:, None, :]) + shift[:, None, :]).astype(jnp.bfloat16)

def attend(query, keys, values):
    length, head_size = query.shape
    block = min(512, length)
    blocks = query.reshape(length // block, block, head_size)

    def one_block(query_rows):
        scores = lax.dot_general(query_rows, keys, (((1,), (1,)), ((), ())), preferred_element_type=jnp.float32)
        scores = scores / math.sqrt(head_size)
        largest = lax.optimization_barrier(jnp.max(scores, axis=1, keepdims=True))
        weights = jnp.exp(scores - largest)
        probs = (weights / lax.optimization_barrier(jnp.sum(weights, axis=1, keepdims=True))).astype(jnp.bfloat16)
        return jnp.dot(probs, values, preferred_element_type=jnp.float32).astype(jnp.bfloat16)
    return lax.map(one_block, blocks).reshape(length, head_size)

def reference(latents, timestep, w_mod, w_qkv, w_out):
    width = latents.shape[2]
    head_size = w_out.shape[1]
    mod = modulation(timestep, w_mod)
    shift = mod[:, :width]
    scale = mod[:, width:2 * width]
    gate = mod[:, 2 * width:]
    normed = normalize(latents, shift, scale)

    def one_image(inputs):
        normed_one, gate_one = inputs

        def one_head(total, weights):
            weight_in, weight_out = weights
            qkv = jnp.dot(normed_one, weight_in, preferred_element_type=jnp.float32).astype(jnp.bfloat16)
            attended = attend(qkv[:, :head_size], qkv[:, head_size:2 * head_size], qkv[:, 2 * head_size:])
            contrib = jnp.dot(attended, weight_out, preferred_element_type=jnp.float32).astype(jnp.bfloat16)
            contrib = lax.optimization_barrier(contrib)
            return (total + contrib.astype(jnp.float32), None)
        start_total = jnp.zeros((normed_one.shape[0], width), jnp.float32)
        total, unused = lax.scan(one_head, start_total, (w_qkv, w_out))
        return (gate_one[None, :] * total).astype(jnp.bfloat16)
    return lax.map(one_image, (normed, gate))
```

```python
import functools
import math

import jax
import jax.numpy as jnp
from jax import lax
from jax.experimental import pallas as pl
from jax.experimental.pallas import tpu as pltpu
from jax.sharding import PartitionSpec as P


AXES = ("grp", "sp")


def modulation(timestep, w_mod):
    half_freq = w_mod.shape[0] // 2
    freqs = jnp.exp(-math.log(10000.0) * jnp.arange(half_freq, dtype=jnp.float32) / half_freq)
    angles = timestep.astype(jnp.float32)[:, None] * freqs[None, :]
    embed = jnp.concatenate([jnp.cos(angles), jnp.sin(angles)], axis=1).astype(jnp.bfloat16)
    return jnp.dot(embed, w_mod, preferred_element_type=jnp.float32)


def normalize(latents, shift, scale):
    values = latents.astype(jnp.float32)
    center = jnp.mean(values, axis=-1, keepdims=True)
    spread = jnp.mean((values - center) ** 2, axis=-1, keepdims=True)
    normed = (values - center) * lax.rsqrt(spread + 1e-06)
    return (normed * (1.0 + scale) + shift).astype(jnp.bfloat16)


def project_kernel(chips, owner_ref, x_ref, *refs):
    pieces, out_ref = refs[:-1], refs[-1]
    total = jnp.zeros(out_ref.shape, jnp.float32)
    for index, piece in enumerate(pieces):
        rows = piece.shape[0]
        start = pl.multiple_of(owner_ref[index] * rows, 128)
        total += jnp.dot(x_ref[:, pl.ds(start, rows)], piece[...], preferred_element_type=jnp.float32)
    out_ref[...] = total.astype(out_ref.dtype)


def project(x, pieces, owners):
    rows, columns = pieces[0].shape
    if rows % 128:
        total = jnp.zeros((x.shape[0], columns), jnp.float32)
        for index, piece in enumerate(pieces):
            part = lax.dynamic_slice_in_dim(x, owners[index] * rows, rows, axis=1)
            total += jnp.dot(part, piece, preferred_element_type=jnp.float32)
        return total.astype(jnp.bfloat16)
    vmem = pl.BlockSpec(memory_space=pltpu.VMEM)
    return pl.pallas_call(
        functools.partial(project_kernel, len(pieces) // 2),
        out_shape=jax.ShapeDtypeStruct((x.shape[0], columns), jnp.bfloat16),
        in_specs=[pl.BlockSpec(memory_space=pltpu.SMEM)] + [vmem] * (1 + len(pieces)),
        out_specs=vmem,
        cost_estimate=pl.CostEstimate(
            flops=2 * x.shape[0] * x.shape[1] * columns,
            bytes_accessed=2 * (x.size + x.shape[1] * columns),
            transcendentals=0,
        ),
    )(owners, x, *pieces)


def attend(query, keys, values):
    head_size = query.shape[1]
    scores = lax.dot_general(query, keys, (((1,), (1,)), ((), ())), preferred_element_type=jnp.float32)
    scores = scores / math.sqrt(head_size)
    largest = jnp.max(scores, axis=1, keepdims=True)
    weights = jnp.exp(scores - largest)
    probs = (weights / jnp.sum(weights, axis=1, keepdims=True)).astype(jnp.bfloat16)
    return jnp.dot(probs, values, preferred_element_type=jnp.float32).astype(jnp.bfloat16)


def on_device(groups, spread, latents, timestep, w_mod, w_qkv, w_out):
    images, tok_local, width = latents.shape
    head_size = w_qkv.shape[2] // 3
    half = spread // 2
    chips = groups // 2
    grp = lax.axis_index("grp")

    def move(value, grp_to, sp_to):
        pairs = []
        for g in range(groups):
            for s in range(spread):
                pairs.append((g * spread + s, grp_to(g) * spread + sp_to(s)))
        return lax.ppermute(value, AXES, pairs)

    def sp_shift(across, along):
        def to(s):
            return (s // half + across) % 2 * half + (s % half + along) % half
        return to

    def chip_step(step):
        if chips & (chips - 1) == 0:
            return lambda g: ((g // 2) ^ step) * 2 + g % 2
        return lambda g: (g // 2 - step) % chips * 2 + g % 2

    def chip_owner(step):
        if chips & (chips - 1) == 0:
            return (grp // 2) ^ step
        return (grp // 2 + step) % chips

    same = lambda index: index
    partner = lambda g: g ^ 1

    def over_chips(value):
        return [value] + [move(value, chip_step(step), same) for step in range(1, chips)]

    def over_cores(pieces):
        return pieces + [move(piece, partner, same) for piece in pieces]

    owners = jnp.stack(
        [chip_owner(step) * 2 + (grp % 2 + flip) % 2 for flip in range(2) for step in range(chips)]
    ).astype(jnp.int32)

    raw = [latents[0]] + [move(latents[0], same, sp_shift(0, -step)) for step in range(1, half)]
    own_in = over_chips(w_qkv[0])
    other_shard = move(w_qkv[0], same, sp_shift(1, 0))
    out_shards = []
    for step in range(half):
        for across in range(2):
            shard = w_out[0]
            if step or across:
                shard = move(shard, same, sp_shift(across, step))
            out_shards.append(shard)

    mod = modulation(timestep, w_mod)
    shift, scale, gate = mod[:, :width], mod[:, width : 2 * width], mod[:, 2 * width :]
    x = jnp.concatenate([normalize(rows, shift, scale) for rows in raw], axis=0)

    other_in = over_chips(other_shard)
    own_pieces = over_cores(own_in)
    out_mine = over_chips(jnp.stack(out_shards))
    other_pieces = over_cores(other_in)
    out_pieces = over_cores(out_mine)

    rows_each = head_size // groups
    column = jnp.arange(head_size, dtype=jnp.int32)
    source = jnp.repeat(owners, rows_each) * rows_each + column % rows_each
    reorder = (column[:, None] == source[None, :]).astype(jnp.bfloat16)

    queries, local_kv, remote_kv = [], [], []
    for pieces in (own_pieces, other_pieces):
        qkv = project(x, pieces, owners)
        queries.append(qkv[:, :head_size])
        values = jnp.dot(qkv[:, 2 * head_size :], reorder, preferred_element_type=jnp.float32)
        kv = jnp.concatenate([qkv[:, head_size : 2 * head_size], values.astype(jnp.bfloat16)], axis=1)
        local_kv.append(kv)
        remote_kv.append(move(kv, same, sp_shift(1, 0)))

    heads = [None, None]
    for index in (1, 0):
        kv = jnp.concatenate([local_kv[index], remote_kv[1 - index]], axis=0)
        heads[index] = attend(queries[index], kv[:, :head_size], kv[:, head_size:])
    both = jnp.concatenate(heads, axis=1)

    mine = []
    for step in range(half):
        part = both[step * tok_local : (step + 1) * tok_local]
        if step:
            part = move(part, same, sp_shift(0, step))
        mine.append(part)
    attended = jnp.concatenate(mine, axis=1)
    rows = jnp.concatenate(out_pieces, axis=1).reshape(attended.shape[1], width)
    total = jnp.dot(attended, rows, preferred_element_type=jnp.float32)
    return (gate * total).astype(jnp.bfloat16)[None]


def solution(mesh):
    placed = (P("grp", "sp", None), P("grp"), P(), P("sp", "grp", None), P("sp", "grp", None))
    body = functools.partial(on_device, mesh.shape["grp"], mesh.shape["sp"])
    return jax.shard_map(
        body, mesh=mesh, in_specs=placed, out_specs=P("grp", "sp", None), check_vma=False
    )
```

```python
import functools
import math

import jax
import jax.numpy as jnp
from jax import lax
from jax.experimental import pallas as pl
from jax.experimental.pallas import tpu as pltpu
from jax.sharding import PartitionSpec as P


AXES = ("grp", "sp")


def modulation(timestep, w_mod):
    half_freq = w_mod.shape[0] // 2
    freqs = jnp.exp(-math.log(10000.0) * jnp.arange(half_freq, dtype=jnp.float32) / half_freq)
    angles = timestep.astype(jnp.float32)[:, None] * freqs[None, :]
    embed = jnp.concatenate([jnp.cos(angles), jnp.sin(angles)], axis=1).astype(jnp.bfloat16)
    return jnp.dot(embed, w_mod, preferred_element_type=jnp.float32)


def normalize(latents, shift, scale):
    values = latents.astype(jnp.float32)
    center = jnp.mean(values, axis=-1, keepdims=True)
    spread = jnp.mean((values - center) ** 2, axis=-1, keepdims=True)
    normed = (values - center) * lax.rsqrt(spread + 1e-06)
    return (normed * (1.0 + scale) + shift).astype(jnp.bfloat16)


def project_kernel(chunks, owner_ref, reorder_ref, *refs):
    xs, pieces, (query_ref, kv_ref) = refs[:chunks], refs[chunks:-2], refs[-2:]
    head_size = query_ref.shape[1]
    tokens = xs[0].shape[0]
    for chunk, x_ref in enumerate(xs):
        total = jnp.zeros((tokens, 3 * head_size), jnp.float32)
        for index, piece in enumerate(pieces):
            rows = piece.shape[0]
            start = pl.multiple_of(owner_ref[index] * rows, 128)
            total += jnp.dot(x_ref[:, pl.ds(start, rows)], piece[...], preferred_element_type=jnp.float32)
        qkv = total.astype(jnp.bfloat16)
        values = jnp.dot(qkv[:, 2 * head_size :], reorder_ref[...], preferred_element_type=jnp.float32)
        place = pl.ds(chunk * tokens, tokens)
        query_ref[place, :] = qkv[:, :head_size]
        kv_ref[place, :head_size] = qkv[:, head_size : 2 * head_size]
        kv_ref[place, head_size:] = values.astype(jnp.bfloat16)


def project(xs, pieces, owners, reorder):
    rows, columns = pieces[0].shape
    head_size = columns // 3
    if rows % 128:
        x = jnp.concatenate(xs, axis=0)
        total = jnp.zeros((x.shape[0], columns), jnp.float32)
        for index, piece in enumerate(pieces):
            part = lax.dynamic_slice_in_dim(x, owners[index] * rows, rows, axis=1)
            total += jnp.dot(part, piece, preferred_element_type=jnp.float32)
        qkv = total.astype(jnp.bfloat16)
        values = jnp.dot(qkv[:, 2 * head_size :], reorder, preferred_element_type=jnp.float32)
        kv = jnp.concatenate([qkv[:, head_size : 2 * head_size], values.astype(jnp.bfloat16)], axis=1)
        return qkv[:, :head_size], kv
    vmem = pl.BlockSpec(memory_space=pltpu.VMEM)
    tokens = sum(x.shape[0] for x in xs)
    return pl.pallas_call(
        functools.partial(project_kernel, len(xs)),
        out_shape=(
            jax.ShapeDtypeStruct((tokens, head_size), jnp.bfloat16),
            jax.ShapeDtypeStruct((tokens, 2 * head_size), jnp.bfloat16),
        ),
        in_specs=[pl.BlockSpec(memory_space=pltpu.SMEM)] + [vmem] * (1 + len(xs) + len(pieces)),
        out_specs=(vmem, vmem),
        compiler_params=pltpu.CompilerParams(vmem_limit_bytes=16 * 2**20),
        cost_estimate=pl.CostEstimate(
            flops=2 * tokens * xs[0].shape[1] * columns,
            bytes_accessed=2 * (tokens + columns) * xs[0].shape[1],
            transcendentals=0,
        ),
    )(owners, reorder, *xs, *pieces)


def after(value, *ready):
    return lax.optimization_barrier((value,) + ready)[0]


def attend(query, keys, values):
    head_size = query.shape[1]
    scores = lax.dot_general(query, keys, (((1,), (1,)), ((), ())), preferred_element_type=jnp.float32)
    scores = scores / math.sqrt(head_size)
    largest = jnp.max(scores, axis=1, keepdims=True)
    weights = jnp.exp(scores - largest)
    probs = (weights / jnp.sum(weights, axis=1, keepdims=True)).astype(jnp.bfloat16)
    return jnp.dot(probs, values, preferred_element_type=jnp.float32).astype(jnp.bfloat16)


def on_device(groups, spread, latents, timestep, w_mod, w_qkv, w_out):
    _, tok_local, width = latents.shape
    head_size = w_qkv.shape[2] // 3
    half = spread // 2
    chips = groups // 2
    grp = lax.axis_index("grp")

    def move(value, grp_to, sp_to):
        pairs = []
        for g in range(groups):
            for s in range(spread):
                pairs.append((g * spread + s, grp_to(g) * spread + sp_to(s)))
        return lax.ppermute(value, AXES, pairs)

    def sp_shift(across, along):
        def to(s):
            return (s // half + across) % 2 * half + (s % half + along) % half

        return to

    def chip_step(step):
        if chips & (chips - 1) == 0:
            return lambda g: ((g // 2) ^ step) * 2 + g % 2
        return lambda g: (g // 2 - step) % chips * 2 + g % 2

    def chip_owner(step):
        if chips & (chips - 1) == 0:
            return (grp // 2) ^ step
        return (grp // 2 + step) % chips

    same = lambda index: index
    partner = lambda g: g ^ 1

    def over_chips(value):
        return [value] + [move(value, chip_step(step), same) for step in range(1, chips)]

    def over_cores(pieces):
        return pieces + [move(piece, partner, same) for piece in pieces]

    owners = jnp.stack(
        [chip_owner(step) * 2 + (grp % 2 + flip) % 2 for flip in range(2) for step in range(chips)]
    ).astype(jnp.int32)

    rows_each = head_size // groups
    column = jnp.arange(head_size, dtype=jnp.int32)
    source = jnp.repeat(owners, rows_each) * rows_each + column % rows_each
    reorder = (column[:, None] == source[None, :]).astype(jnp.bfloat16)

    raw = [latents[0]] + [move(latents[0], same, sp_shift(0, -step)) for step in range(1, half)]
    other_shard = move(w_qkv[0], same, sp_shift(1, 0))
    own_in = over_chips(w_qkv[0])

    mod = modulation(timestep, w_mod)
    shift, scale, gate = mod[:, :width], mod[:, width : 2 * width], mod[:, 2 * width :]
    mine_normed = normalize(raw[0], shift, scale)

    other_in = over_chips(after(other_shard, mine_normed))
    own_pieces = over_cores(own_in)
    out_shards = []
    out_shard = after(w_out[0], mine_normed)
    for step in range(half):
        for across in range(2):
            shard = out_shard
            if step or across:
                shard = move(shard, same, sp_shift(across, step))
            out_shards.append(shard)

    xs = [mine_normed] + [normalize(rows, shift, scale) for rows in after(raw, mine_normed)[1:]]

    queries, local_kv, remote_kv = [], [], []
    for pieces in (own_pieces, None):
        if pieces is None:
            other_in = after(other_in, local_kv[0])
            out_mine = over_chips(after(jnp.stack(out_shards), local_kv[0]))
            pieces = over_cores(other_in)
        query, kv = project(xs, pieces, owners, reorder)
        queries.append(query)
        local_kv.append(kv)
        remote_kv.append(move(kv, same, sp_shift(1, 0)))
    out_pieces = over_cores(after(out_mine, local_kv[1]))

    heads = [None, None]
    for index in (1, 0):
        kv = jnp.concatenate([local_kv[index], remote_kv[1 - index]], axis=0)
        heads[index] = attend(queries[index], kv[:, :head_size], kv[:, head_size:])
    both = jnp.concatenate(heads, axis=1)

    mine = []
    for step in range(half):
        part = both[step * tok_local : (step + 1) * tok_local]
        if step:
            part = move(part, same, sp_shift(0, step))
        mine.append(part)
    attended = jnp.concatenate(mine, axis=1)
    rows = jnp.concatenate(out_pieces, axis=1).reshape(attended.shape[1], width)
    total = jnp.dot(attended, rows, preferred_element_type=jnp.float32)
    return (gate * total).astype(jnp.bfloat16)[None]


def solution(mesh):
    placed = (P("grp", "sp", None), P("grp"), P(), P("sp", "grp", None), P("sp", "grp", None))

    def body(*args):
        return on_device(mesh.shape["grp"], mesh.shape["sp"], *args)

    return jax.shard_map(
        body, mesh=mesh, in_specs=placed, out_specs=P("grp", "sp", None), check_vma=False
    )
```

```python
import functools
import math

import jax
import jax.numpy as jnp
from jax import lax
from jax.experimental import pallas as pl
from jax.experimental.pallas import tpu as pltpu
from jax.sharding import PartitionSpec as P


AXES = ("grp", "sp")


def modulation(timestep, w_mod):
    half_freq = w_mod.shape[0] // 2
    freqs = jnp.exp(-math.log(10000.0) * jnp.arange(half_freq, dtype=jnp.float32) / half_freq)
    angles = timestep.astype(jnp.float32)[:, None] * freqs[None, :]
    embed = jnp.concatenate([jnp.cos(angles), jnp.sin(angles)], axis=1).astype(jnp.bfloat16)
    return jnp.dot(embed, w_mod, preferred_element_type=jnp.float32)


def normalize_kernel(block, x_ref, shift_ref, scale_ref, out_ref):
    gain = 1.0 + scale_ref[...]
    shift = shift_ref[...]

    @pl.loop(0, x_ref.shape[0] // block)
    def _(step):
        rows = pl.ds(pl.multiple_of(step * block, block), block)
        values = x_ref[rows, :].astype(jnp.float32)
        centered = values - jnp.mean(values, axis=-1, keepdims=True)
        spread = jnp.mean(centered * centered, axis=-1, keepdims=True)
        out_ref[rows, :] = (centered * lax.rsqrt(spread + 1e-06) * gain + shift).astype(out_ref.dtype)


def normalize(rows, shift, scale):
    vmem = pl.BlockSpec(memory_space=pltpu.VMEM)
    block = math.gcd(rows.shape[0], 32)
    return pl.pallas_call(
        functools.partial(normalize_kernel, block),
        out_shape=jax.ShapeDtypeStruct(rows.shape, jnp.bfloat16),
        in_specs=[vmem] * 3,
        out_specs=vmem,
        compiler_params=pltpu.CompilerParams(vmem_limit_bytes=8 * 2**20),
        cost_estimate=pl.CostEstimate(
            flops=10 * rows.size, bytes_accessed=4 * rows.size, transcendentals=0
        ),
    )(rows, shift, scale)


def project_kernel(chunks, owner_ref, reorder_ref, *refs):
    xs, pieces, (query_ref, kv_ref) = refs[:chunks], refs[chunks:-2], refs[-2:]
    head_size = query_ref.shape[1]
    tokens = xs[0].shape[0]
    for chunk, x_ref in enumerate(xs):
        total = jnp.zeros((tokens, 3 * head_size), jnp.float32)
        for index, piece in enumerate(pieces):
            rows = piece.shape[0]
            start = pl.multiple_of(owner_ref[index] * rows, 128)
            total += jnp.dot(x_ref[:, pl.ds(start, rows)], piece[...], preferred_element_type=jnp.float32)
        qkv = total.astype(jnp.bfloat16)
        values = jnp.dot(qkv[:, 2 * head_size :], reorder_ref[...], preferred_element_type=jnp.float32)
        place = pl.ds(chunk * tokens, tokens)
        query_ref[place, :] = qkv[:, :head_size]
        kv_ref[place, :head_size] = qkv[:, head_size : 2 * head_size]
        kv_ref[place, head_size:] = values.astype(jnp.bfloat16)


def project(xs, pieces, owners, reorder):
    rows, columns = pieces[0].shape
    head_size = columns // 3
    if rows % 128:
        x = jnp.concatenate(xs, axis=0)
        total = jnp.zeros((x.shape[0], columns), jnp.float32)
        for index, piece in enumerate(pieces):
            part = lax.dynamic_slice_in_dim(x, owners[index] * rows, rows, axis=1)
            total += jnp.dot(part, piece, preferred_element_type=jnp.float32)
        qkv = total.astype(jnp.bfloat16)
        values = jnp.dot(qkv[:, 2 * head_size :], reorder, preferred_element_type=jnp.float32)
        kv = jnp.concatenate([qkv[:, head_size : 2 * head_size], values.astype(jnp.bfloat16)], axis=1)
        return qkv[:, :head_size], kv
    vmem = pl.BlockSpec(memory_space=pltpu.VMEM)
    tokens = sum(x.shape[0] for x in xs)
    return pl.pallas_call(
        functools.partial(project_kernel, len(xs)),
        out_shape=(
            jax.ShapeDtypeStruct((tokens, head_size), jnp.bfloat16),
            jax.ShapeDtypeStruct((tokens, 2 * head_size), jnp.bfloat16),
        ),
        in_specs=[pl.BlockSpec(memory_space=pltpu.SMEM)] + [vmem] * (1 + len(xs) + len(pieces)),
        out_specs=(vmem, vmem),
        compiler_params=pltpu.CompilerParams(vmem_limit_bytes=16 * 2**20),
        cost_estimate=pl.CostEstimate(
            flops=2 * tokens * xs[0].shape[1] * columns,
            bytes_accessed=2 * (tokens + columns) * xs[0].shape[1],
            transcendentals=0,
        ),
    )(owners, reorder, *xs, *pieces)


def after(value, *ready):
    return lax.optimization_barrier((value,) + ready)[0]


def attend(query, keys, values):
    head_size = query.shape[1]
    scores = lax.dot_general(query, keys, (((1,), (1,)), ((), ())), preferred_element_type=jnp.float32)
    scores = scores / math.sqrt(head_size)
    largest = jnp.max(scores, axis=1, keepdims=True)
    weights = jnp.exp(scores - largest)
    probs = (weights / jnp.sum(weights, axis=1, keepdims=True)).astype(jnp.bfloat16)
    return jnp.dot(probs, values, preferred_element_type=jnp.float32).astype(jnp.bfloat16)


def on_device(groups, spread, latents, timestep, w_mod, w_qkv, w_out):
    _, tok_local, width = latents.shape
    head_size = w_qkv.shape[2] // 3
    half = spread // 2
    chips = groups // 2
    grp = lax.axis_index("grp")

    def move(value, grp_to, sp_to):
        pairs = []
        for g in range(groups):
            for s in range(spread):
                pairs.append((g * spread + s, grp_to(g) * spread + sp_to(s)))
        return lax.ppermute(value, AXES, pairs)

    def sp_shift(across, along):
        def to(s):
            return (s // half + across) % 2 * half + (s % half + along) % half

        return to

    def chip_step(step):
        if chips & (chips - 1) == 0:
            return lambda g: ((g // 2) ^ step) * 2 + g % 2
        return lambda g: (g // 2 - step) % chips * 2 + g % 2

    def chip_owner(step):
        if chips & (chips - 1) == 0:
            return (grp // 2) ^ step
        return (grp // 2 + step) % chips

    same = lambda index: index
    partner = lambda g: g ^ 1

    def over_chips(value):
        return [value] + [move(value, chip_step(step), same) for step in range(1, chips)]

    def over_cores(pieces):
        return pieces + [move(piece, partner, same) for piece in pieces]

    owners = jnp.stack(
        [chip_owner(step) * 2 + (grp % 2 + flip) % 2 for flip in range(2) for step in range(chips)]
    ).astype(jnp.int32)

    rows_each = head_size // groups
    column = jnp.arange(head_size, dtype=jnp.int32)
    source = jnp.repeat(owners, rows_each) * rows_each + column % rows_each
    reorder = (column[:, None] == source[None, :]).astype(jnp.bfloat16)

    raw = [latents[0]] + [move(latents[0], same, sp_shift(0, -step)) for step in range(1, half)]
    other_shard = move(w_qkv[0], same, sp_shift(1, 0))
    own_in = over_chips(w_qkv[0])

    mod = modulation(timestep, w_mod)
    shift, scale, gate = mod[:, :width], mod[:, width : 2 * width], mod[:, 2 * width :]
    mine_normed = normalize(raw[0], shift, scale)

    other_in = over_chips(after(other_shard, mine_normed))
    own_pieces = over_cores(own_in)
    out_shards = []
    out_shard = after(w_out[0], mine_normed)
    for step in range(half):
        for across in range(2):
            shard = out_shard
            if step or across:
                shard = move(shard, same, sp_shift(across, step))
            out_shards.append(shard)

    xs = [mine_normed] + [normalize(rows, shift, scale) for rows in after(raw, mine_normed)[1:]]

    query_0, kv_0 = project(xs, own_pieces, owners, reorder)
    remote_0 = move(kv_0, same, sp_shift(1, 0))
    out_mine = over_chips(after(jnp.stack(out_shards), kv_0))
    other_in = after(other_in, kv_0)
    other_pieces = over_cores(other_in)
    query_1, kv_1 = project(xs, other_pieces, owners, reorder)
    remote_1 = move(kv_1, same, sp_shift(1, 0))
    out_pieces = over_cores(after(out_mine, kv_1))
    queries, local_kv, remote_kv = [query_0, query_1], [kv_0, kv_1], [remote_0, remote_1]

    heads = [None, None]
    for index in (1, 0):
        kv = jnp.concatenate([local_kv[index], remote_kv[1 - index]], axis=0)
        heads[index] = attend(queries[index], kv[:, :head_size], kv[:, head_size:])
    both = jnp.concatenate(heads, axis=1)

    mine = []
    for step in range(half):
        part = both[step * tok_local : (step + 1) * tok_local]
        if step:
            part = move(part, same, sp_shift(0, step))
        mine.append(part)
    attended = jnp.concatenate(mine, axis=1)
    rows = jnp.concatenate(out_pieces, axis=1).reshape(attended.shape[1], width)
    total = jnp.dot(attended, rows, preferred_element_type=jnp.float32)
    return (gate * total).astype(jnp.bfloat16)[None]


def solution(mesh):
    placed = (P("grp", "sp", None), P("grp"), P(), P("sp", "grp", None), P("sp", "grp", None))

    def body(*args):
        return on_device(mesh.shape["grp"], mesh.shape["sp"], *args)

    return jax.shard_map(
        body, mesh=mesh, in_specs=placed, out_specs=P("grp", "sp", None), check_vma=False
    )
```

```python
import functools
import math

import jax
import jax.numpy as jnp
from jax import lax
from jax.experimental import pallas as pl
from jax.experimental.pallas import tpu as pltpu
from jax.sharding import PartitionSpec as P


AXES = ("grp", "sp")


def modulation(timestep, w_mod):
    half_freq = w_mod.shape[0] // 2
    freqs = jnp.exp(-math.log(10000.0) * jnp.arange(half_freq, dtype=jnp.float32) / half_freq)
    angles = timestep.astype(jnp.float32)[:, None] * freqs[None, :]
    embed = jnp.concatenate([jnp.cos(angles), jnp.sin(angles)], axis=1).astype(jnp.bfloat16)
    return jnp.dot(embed, w_mod, preferred_element_type=jnp.float32)


def normalize_kernel(block, x_ref, shift_ref, scale_ref, out_ref):
    gain = 1.0 + scale_ref[...]
    shift = shift_ref[...]

    @pl.loop(0, x_ref.shape[0] // block)
    def _(step):
        rows = pl.ds(pl.multiple_of(step * block, block), block)
        values = x_ref[rows, :].astype(jnp.float32)
        centered = values - jnp.mean(values, axis=-1, keepdims=True)
        spread = jnp.mean(centered * centered, axis=-1, keepdims=True)
        out_ref[rows, :] = (centered * lax.rsqrt(spread + 1e-06) * gain + shift).astype(out_ref.dtype)


def normalize(rows, shift, scale):
    vmem = pl.BlockSpec(memory_space=pltpu.VMEM)
    block = math.gcd(rows.shape[0], 32)
    return pl.pallas_call(
        functools.partial(normalize_kernel, block),
        out_shape=jax.ShapeDtypeStruct(rows.shape, jnp.bfloat16),
        in_specs=[vmem] * 3,
        out_specs=vmem,
        compiler_params=pltpu.CompilerParams(vmem_limit_bytes=8 * 2**20),
        cost_estimate=pl.CostEstimate(
            flops=10 * rows.size, bytes_accessed=4 * rows.size, transcendentals=0
        ),
    )(rows, shift, scale)


def project_kernel(chunks, owner_ref, reorder_ref, *refs):
    xs, pieces, (query_ref, kv_ref) = refs[:chunks], refs[chunks:-2], refs[-2:]
    head_size = query_ref.shape[1]
    tokens = xs[0].shape[0]
    for chunk, x_ref in enumerate(xs):
        total = jnp.zeros((tokens, 3 * head_size), jnp.float32)
        for index, piece in enumerate(pieces):
            rows = piece.shape[0]
            start = pl.multiple_of(owner_ref[index] * rows, 128)
            total += jnp.dot(x_ref[:, pl.ds(start, rows)], piece[...], preferred_element_type=jnp.float32)
        qkv = total.astype(jnp.bfloat16)
        values = jnp.dot(qkv[:, 2 * head_size :], reorder_ref[...], preferred_element_type=jnp.float32)
        place = pl.ds(chunk * tokens, tokens)
        query_ref[place, :] = qkv[:, :head_size]
        kv_ref[place, :head_size] = qkv[:, head_size : 2 * head_size]
        kv_ref[place, head_size:] = values.astype(jnp.bfloat16)


def project(xs, pieces, owners, reorder):
    rows, columns = pieces[0].shape
    head_size = columns // 3
    if rows % 128:
        x = jnp.concatenate(xs, axis=0)
        total = jnp.zeros((x.shape[0], columns), jnp.float32)
        for index, piece in enumerate(pieces):
            part = lax.dynamic_slice_in_dim(x, owners[index] * rows, rows, axis=1)
            total += jnp.dot(part, piece, preferred_element_type=jnp.float32)
        qkv = total.astype(jnp.bfloat16)
        values = jnp.dot(qkv[:, 2 * head_size :], reorder, preferred_element_type=jnp.float32)
        kv = jnp.concatenate([qkv[:, head_size : 2 * head_size], values.astype(jnp.bfloat16)], axis=1)
        return qkv[:, :head_size], kv
    vmem = pl.BlockSpec(memory_space=pltpu.VMEM)
    tokens = sum(x.shape[0] for x in xs)
    return pl.pallas_call(
        functools.partial(project_kernel, len(xs)),
        out_shape=(
            jax.ShapeDtypeStruct((tokens, head_size), jnp.bfloat16),
            jax.ShapeDtypeStruct((tokens, 2 * head_size), jnp.bfloat16),
        ),
        in_specs=[pl.BlockSpec(memory_space=pltpu.SMEM)] + [vmem] * (1 + len(xs) + len(pieces)),
        out_specs=(vmem, vmem),
        compiler_params=pltpu.CompilerParams(vmem_limit_bytes=16 * 2**20),
        cost_estimate=pl.CostEstimate(
            flops=2 * tokens * xs[0].shape[1] * columns,
            bytes_accessed=2 * (tokens + columns) * xs[0].shape[1],
            transcendentals=0,
        ),
    )(owners, reorder, *xs, *pieces)


def after(value, *ready):
    return lax.optimization_barrier((value,) + ready)[0]


def attend(query, keys, values):
    head_size = query.shape[1]
    scores = lax.dot_general(query, keys, (((1,), (1,)), ((), ())), preferred_element_type=jnp.float32)
    scores = scores / math.sqrt(head_size)
    largest = jnp.max(scores, axis=1, keepdims=True)
    weights = jnp.exp(scores - largest)
    probs = (weights / jnp.sum(weights, axis=1, keepdims=True)).astype(jnp.bfloat16)
    return jnp.dot(probs, values, preferred_element_type=jnp.float32).astype(jnp.bfloat16)


def on_device(groups, spread, latents, timestep, w_mod, w_qkv, w_out):
    _, tok_local, width = latents.shape
    head_size = w_qkv.shape[2] // 3
    half = spread // 2
    chips = groups // 2
    grp = lax.axis_index("grp")

    def move(value, grp_to, sp_to):
        pairs = []
        for g in range(groups):
            for s in range(spread):
                pairs.append((g * spread + s, grp_to(g) * spread + sp_to(s)))
        return lax.ppermute(value, AXES, pairs)

    def sp_shift(across, along):
        def to(s):
            return (s // half + across) % 2 * half + (s % half + along) % half

        return to

    def chip_step(step):
        if chips & (chips - 1) == 0:
            return lambda g: ((g // 2) ^ step) * 2 + g % 2
        return lambda g: (g // 2 - step) % chips * 2 + g % 2

    def chip_owner(step):
        if chips & (chips - 1) == 0:
            return (grp // 2) ^ step
        return (grp // 2 + step) % chips

    same = lambda index: index
    partner = lambda g: g ^ 1

    def over_chips(value):
        return [value] + [move(value, chip_step(step), same) for step in range(1, chips)]

    def over_cores(pieces):
        return pieces + [move(piece, partner, same) for piece in pieces]

    owners = jnp.stack(
        [chip_owner(step) * 2 + (grp % 2 + flip) % 2 for flip in range(2) for step in range(chips)]
    ).astype(jnp.int32)

    rows_each = head_size // groups
    column = jnp.arange(head_size, dtype=jnp.int32)
    source = jnp.repeat(owners, rows_each) * rows_each + column % rows_each
    reorder = (column[:, None] == source[None, :]).astype(jnp.bfloat16)

    other_shard = move(w_qkv[0], same, sp_shift(1, 0))
    own_in = over_chips(w_qkv[0])
    out_shards = []
    for step in range(half):
        for across in range(2):
            shard = w_out[0]
            if step or across:
                shard = move(shard, same, sp_shift(across, step))
            out_shards.append(shard)
    raw = [move(latents[0], same, sp_shift(0, -step)) for step in range(1, half)]

    mod = modulation(timestep, w_mod)
    shift, scale, gate = mod[:, :width], mod[:, width : 2 * width], mod[:, 2 * width :]
    mine_normed = normalize(latents[0], shift, scale)

    other_in = over_chips(after(other_shard, mine_normed))
    own_pieces = over_cores(own_in)
    out_mine = over_chips(after(jnp.stack(out_shards), mine_normed))
    query_own, kv_own = project([mine_normed], own_pieces, owners, reorder)
    other_pieces = over_cores(after(other_in, kv_own))

    queries, local_kv, remote_kv = [[], []], [], []
    for stage in range(2):
        if stage:
            raw = after(raw, local_kv[0])
            xs = [normalize(rows, shift, scale) for rows in raw]
            query_own, kv_own = project(xs, own_pieces, owners, reorder)
        else:
            xs = [mine_normed]
        query_other, kv_other = project(xs, other_pieces, owners, reorder)
        queries[0].append(query_own)
        queries[1].append(query_other)
        local_kv.append(jnp.concatenate([kv_own, kv_other], axis=1))
        remote_kv.append(move(local_kv[-1], same, sp_shift(1, 0)))
    heads = []
    for index in range(2):
        here = index * 2 * head_size
        there = (1 - index) * 2 * head_size
        keys = [kv[:, here : here + head_size] for kv in local_kv]
        keys += [kv[:, there : there + head_size] for kv in remote_kv]
        values = [kv[:, here + head_size : here + 2 * head_size] for kv in local_kv]
        values += [kv[:, there + head_size : there + 2 * head_size] for kv in remote_kv]
        heads.append(
            attend(
                jnp.concatenate(queries[index], axis=0),
                jnp.concatenate(keys, axis=0),
                jnp.concatenate(values, axis=0),
            )
        )
    both = jnp.concatenate(heads, axis=1)

    mine = []
    for step in range(half):
        part = both[step * tok_local : (step + 1) * tok_local]
        if step:
            part = move(part, same, sp_shift(0, step))
        mine.append(part)
    out_pieces = over_cores(after(out_mine, both))
    attended = jnp.concatenate(mine, axis=1)
    rows = jnp.concatenate(out_pieces, axis=1).reshape(attended.shape[1], width)
    total = jnp.dot(attended, rows, preferred_element_type=jnp.float32)
    return (gate * total).astype(jnp.bfloat16)[None]


def solution(mesh):
    placed = (P("grp", "sp", None), P("grp"), P(), P("sp", "grp", None), P("sp", "grp", None))

    def body(*args):
        return on_device(mesh.shape["grp"], mesh.shape["sp"], *args)

    return jax.shard_map(
        body, mesh=mesh, in_specs=placed, out_specs=P("grp", "sp", None), check_vma=False
    )
```

```python
import functools
import math

import jax
import jax.numpy as jnp
from jax import lax
from jax.experimental import pallas as pl
from jax.experimental.pallas import tpu as pltpu
from jax.sharding import PartitionSpec as P


AXES = ("grp", "sp")


def modulation(timestep, w_mod):
    half_freq = w_mod.shape[0] // 2
    freqs = jnp.exp(-math.log(10000.0) * jnp.arange(half_freq, dtype=jnp.float32) / half_freq)
    angles = timestep.astype(jnp.float32)[:, None] * freqs[None, :]
    embed = jnp.concatenate([jnp.cos(angles), jnp.sin(angles)], axis=1).astype(jnp.bfloat16)
    return jnp.dot(embed, w_mod, preferred_element_type=jnp.float32)


def normalize_kernel(block, x_ref, shift_ref, scale_ref, out_ref):
    gain = 1.0 + scale_ref[...]
    shift = shift_ref[...]

    @pl.loop(0, x_ref.shape[0] // block)
    def _(step):
        rows = pl.ds(pl.multiple_of(step * block, block), block)
        values = x_ref[rows, :].astype(jnp.float32)
        centered = values - jnp.mean(values, axis=-1, keepdims=True)
        spread = jnp.mean(centered * centered, axis=-1, keepdims=True)
        out_ref[rows, :] = (centered * lax.rsqrt(spread + 1e-06) * gain + shift).astype(out_ref.dtype)


def normalize(rows, shift, scale):
    vmem = pl.BlockSpec(memory_space=pltpu.VMEM)
    block = math.gcd(rows.shape[0], 32)
    return pl.pallas_call(
        functools.partial(normalize_kernel, block),
        out_shape=jax.ShapeDtypeStruct(rows.shape, jnp.bfloat16),
        in_specs=[vmem] * 3,
        out_specs=vmem,
        compiler_params=pltpu.CompilerParams(vmem_limit_bytes=8 * 2**20),
        cost_estimate=pl.CostEstimate(
            flops=10 * rows.size, bytes_accessed=4 * rows.size, transcendentals=0
        ),
    )(rows, shift, scale)


def project_kernel(chunks, owner_ref, reorder_ref, *refs):
    xs, pieces, (query_ref, kv_ref) = refs[:chunks], refs[chunks:-2], refs[-2:]
    head_size = query_ref.shape[1]
    tokens = xs[0].shape[0]
    for chunk, x_ref in enumerate(xs):
        total = jnp.zeros((tokens, 3 * head_size), jnp.float32)
        for index, piece in enumerate(pieces):
            rows = piece.shape[0]
            start = pl.multiple_of(owner_ref[index] * rows, 128)
            total += jnp.dot(x_ref[:, pl.ds(start, rows)], piece[...], preferred_element_type=jnp.float32)
        qkv = total.astype(jnp.bfloat16)
        values = jnp.dot(qkv[:, 2 * head_size :], reorder_ref[...], preferred_element_type=jnp.float32)
        place = pl.ds(chunk * tokens, tokens)
        query_ref[place, :] = qkv[:, :head_size]
        kv_ref[place, :head_size] = qkv[:, head_size : 2 * head_size]
        kv_ref[place, head_size:] = values.astype(jnp.bfloat16)


def project(xs, pieces, owners, reorder):
    rows, columns = pieces[0].shape
    head_size = columns // 3
    if rows % 128:
        x = jnp.concatenate(xs, axis=0)
        total = jnp.zeros((x.shape[0], columns), jnp.float32)
        for index, piece in enumerate(pieces):
            part = lax.dynamic_slice_in_dim(x, owners[index] * rows, rows, axis=1)
            total += jnp.dot(part, piece, preferred_element_type=jnp.float32)
        qkv = total.astype(jnp.bfloat16)
        values = jnp.dot(qkv[:, 2 * head_size :], reorder, preferred_element_type=jnp.float32)
        kv = jnp.concatenate([qkv[:, head_size : 2 * head_size], values.astype(jnp.bfloat16)], axis=1)
        return qkv[:, :head_size], kv
    vmem = pl.BlockSpec(memory_space=pltpu.VMEM)
    tokens = sum(x.shape[0] for x in xs)
    return pl.pallas_call(
        functools.partial(project_kernel, len(xs)),
        out_shape=(
            jax.ShapeDtypeStruct((tokens, head_size), jnp.bfloat16),
            jax.ShapeDtypeStruct((tokens, 2 * head_size), jnp.bfloat16),
        ),
        in_specs=[pl.BlockSpec(memory_space=pltpu.SMEM)] + [vmem] * (1 + len(xs) + len(pieces)),
        out_specs=(vmem, vmem),
        compiler_params=pltpu.CompilerParams(vmem_limit_bytes=16 * 2**20),
        cost_estimate=pl.CostEstimate(
            flops=2 * tokens * xs[0].shape[1] * columns,
            bytes_accessed=2 * (tokens + columns) * xs[0].shape[1],
            transcendentals=0,
        ),
    )(owners, reorder, *xs, *pieces)


def after(value, *ready):
    return lax.optimization_barrier((value,) + ready)[0]


def attend(query, keys, values):
    head_size = query.shape[1]
    scores = lax.dot_general(query, keys, (((1,), (1,)), ((), ())), preferred_element_type=jnp.float32)
    scores = scores / math.sqrt(head_size)
    largest = jnp.max(scores, axis=1, keepdims=True)
    weights = jnp.exp(scores - largest)
    probs = (weights / jnp.sum(weights, axis=1, keepdims=True)).astype(jnp.bfloat16)
    return jnp.dot(probs, values, preferred_element_type=jnp.float32).astype(jnp.bfloat16)


def on_device(groups, spread, latents, timestep, w_mod, w_qkv, w_out):
    _, tok_local, width = latents.shape
    head_size = w_qkv.shape[2] // 3
    half = spread // 2
    chips = groups // 2
    grp = lax.axis_index("grp")

    def move(value, grp_to, sp_to):
        pairs = []
        for g in range(groups):
            for s in range(spread):
                pairs.append((g * spread + s, grp_to(g) * spread + sp_to(s)))
        return lax.ppermute(value, AXES, pairs)

    def sp_shift(across, along):
        def to(s):
            return (s // half + across) % 2 * half + (s % half + along) % half

        return to

    def chip_step(step):
        if chips & (chips - 1) == 0:
            return lambda g: ((g // 2) ^ step) * 2 + g % 2
        return lambda g: (g // 2 - step) % chips * 2 + g % 2

    def chip_owner(step):
        if chips & (chips - 1) == 0:
            return (grp // 2) ^ step
        return (grp // 2 + step) % chips

    same = lambda index: index
    partner = lambda g: g ^ 1

    def over_chips(value):
        return [value] + [move(value, chip_step(step), same) for step in range(1, chips)]

    def over_cores(pieces):
        return pieces + [move(piece, partner, same) for piece in pieces]

    owners = jnp.stack(
        [chip_owner(step) * 2 + (grp % 2 + flip) % 2 for flip in range(2) for step in range(chips)]
    ).astype(jnp.int32)

    rows_each = head_size // groups
    column = jnp.arange(head_size, dtype=jnp.int32)
    source = jnp.repeat(owners, rows_each) * rows_each + column % rows_each
    reorder = (column[:, None] == source[None, :]).astype(jnp.bfloat16)

    other_shard = move(w_qkv[0], same, sp_shift(1, 0))
    own_in = over_chips(w_qkv[0])
    out_shards = []
    for step in range(half):
        for across in range(2):
            shard = w_out[0]
            if step or across:
                shard = move(shard, same, sp_shift(across, step))
            out_shards.append(shard)
    raw = [move(latents[0], same, sp_shift(0, -step)) for step in range(1, half)]

    mod = modulation(timestep, w_mod)
    shift, scale, gate = mod[:, :width], mod[:, width : 2 * width], mod[:, 2 * width :]
    mine_normed = normalize(latents[0], shift, scale)

    other_in = over_chips(after(other_shard, mine_normed))
    own_pieces = over_cores(own_in)
    out_mine = over_chips(after(jnp.stack(out_shards), mine_normed))
    query_mine, kv_mine = project([mine_normed], own_pieces, owners, reorder)
    remote_mine = move(kv_mine, same, sp_shift(1, 0))
    rest = [normalize(rows, shift, scale) for rows in after(raw, kv_mine)]
    query_rest, kv_rest = project(rest, own_pieces, owners, reorder)
    remote_rest = move(kv_rest, same, sp_shift(1, 0))
    other_pieces = over_cores(after(other_in, kv_rest))
    query_other, kv_other = project([mine_normed] + rest, other_pieces, owners, reorder)
    remote_other = move(kv_other, same, sp_shift(1, 0))

    query_both = jnp.concatenate([query_mine, query_rest], axis=0)
    heads = []
    for query, parts in (
        (query_both, [kv_mine, kv_rest, remote_other]),
        (query_other, [kv_other, remote_mine, remote_rest]),
    ):
        kv = jnp.concatenate(parts, axis=0)
        heads.append(attend(query, kv[:, :head_size], kv[:, head_size:]))
    both = jnp.concatenate(heads, axis=1)

    mine = []
    for step in range(half):
        part = both[step * tok_local : (step + 1) * tok_local]
        if step:
            part = move(part, same, sp_shift(0, step))
        mine.append(part)
    out_pieces = over_cores(after(out_mine, both))
    attended = jnp.concatenate(mine, axis=1)
    rows = jnp.concatenate(out_pieces, axis=1).reshape(attended.shape[1], width)
    total = jnp.dot(attended, rows, preferred_element_type=jnp.float32)
    return (gate * total).astype(jnp.bfloat16)[None]


def solution(mesh):
    placed = (P("grp", "sp", None), P("grp"), P(), P("sp", "grp", None), P("sp", "grp", None))

    def body(*args):
        return on_device(mesh.shape["grp"], mesh.shape["sp"], *args)

    return jax.shard_map(
        body, mesh=mesh, in_specs=placed, out_specs=P("grp", "sp", None), check_vma=False
    )
```
